32 devices in a mesh: dp: 4 (over y, core), lat: 4 (over z), chan: 2 (over x).
Axes of the slice: x: 2, y: 2, z: 4, core: 2. Of those that a mesh axis runs over, the one named last changes fastest.
Arguments:
- saved_input: bfloat16 [4, 16, 720, 1024], P('dp', None, 'lat', 'chan'), may hold values from -6 to 6
- grad_output: bfloat16 [4, 16, 720, 1024], P('dp', None, 'lat', 'chan'), may hold values from -6 to 6
- legendre: bfloat16 [16, 192, 720], P('lat'), may hold values from -0.21875 to 0.21875
- quad_weight: float32 [720], replicated, may hold values from 0.3 to 3
- mixing_weight: bfloat16 [192, 512, 1024], P('lat', None, 'chan'), may hold values from -0.375 to 0.375
Outputs:
- grad_weight: bfloat16 [192, 512, 1024], P('lat', 'dp', 'chan')
- grad_input: bfloat16 [4, 16, 720, 1024], P('dp', None, 'lat', 'chan')
The draws below stay inside these ranges and needn't reach their ends.
All inputs are finite; a program needn't handle non-finite values.
Results may differ from the reference program's by a relative error of at most 0.014.
Values may be sent and summed in bfloat16 or wider, within the bound.
A program may use at most 192 MiB of HBM per device.

```python
import math
import jax
import jax.numpy as jnp
from jax import lax

NLAT = 720
L = 192
C = 512
BATCH = 4
M = 16
N_DP = 4
N_CHAN = 2


def strengthened(result, rng, source, target, blocks, factor):
    def block_of(axis_at):
        return (jnp.arange(result.shape[axis_at]) // (result.shape[axis_at] // blocks)).reshape((-1,) + (1,) * (result.ndim - 1 - axis_at))

    first = jax.random.permutation(rng, blocks)[block_of(target)]
    other_side = (block_of(target) + blocks // 2) % blocks
    return jnp.where((block_of(source) == first) | (block_of(source) == other_side), factor * result, result)


def level_of(rng, extent, split, low, top_value):
    def one(axis_at, blocks):
        draws = jax.random.uniform(jax.random.fold_in(jax.random.fold_in(rng, 6), axis_at), (blocks,), jnp.float32, low / len(split), top_value / len(split))
        return jnp.repeat(jnp.exp(draws), extent[axis_at] // blocks).reshape((-1,) + (1,) * (len(extent) - axis_at - 1))

    gain = one(*split[0])
    for cut in split[1:]:
        gain = gain * one(*cut)
    return gain


def gaussian(key, shape, scale, limit, shards=(), held_as=jnp.bfloat16):
    factor_of = level_of(key, shape, shards, -0.22, 0.18) if shards else 1.0
    values = jax.random.normal(key, shape, jnp.float32) * scale * factor_of
    return jnp.minimum(jnp.maximum(values, -limit), limit).astype(held_as)


def bell_draw_with(stream_key, extent, deviation, limit, split, heavy, dtype=jnp.bfloat16):
    values = deviation * jax.random.normal(stream_key, extent, jnp.float32)
    if split:
        values = values * level_of(stream_key, extent, split, -0.22, 0.18)
    return jnp.clip(strengthened(values, jax.random.fold_in(stream_key, 3), *heavy), -limit, limit).astype(dtype)


def setup_inputs(seed: int = 0) -> dict:
    key_list = jax.random.split(jax.random.key(seed), 6)
    saved_input = bell_draw_with(key_list[0], (BATCH, M, NLAT, 2 * C), 1.0, 6.0, ((0, 4), (2, 4), (3, 2)), (0, 3, 4, 2.0))
    grad_output = gaussian(key_list[1], (BATCH, M, NLAT, 2 * C), 1.0, 6.0, ((0, 4), (2, 4), (3, 2)))
    legendre = gaussian(key_list[2], (M, L, NLAT), NLAT ** -0.5, 0.21875, ((0, 4),))
    quad_weight = jnp.clip(jnp.exp(jax.random.uniform(key_list[3], (NLAT,), jnp.float32, math.log(0.3), math.log(3.0))), 0.3, 3.0)
    mixing_weight = bell_draw_with(key_list[4], (L, C, 2 * C), C ** -0.5, 0.375, ((0, 4), (2, 2)), (2, 1, 2, 2.0))
    return {"saved_input": saved_input, "grad_output": grad_output, "legendre": legendre, "quad_weight": quad_weight, "mixing_weight": mixing_weight}


def partner_of(grads):
    pairs = grads.reshape(grads.shape[:-1] + (grads.shape[-1] // 2, 2))
    swapped = jnp.stack([pairs[..., 1], -pairs[..., 0]], axis=-1)
    return swapped.reshape(grads.shape)


def weight_terms(spectra, grads):
    pairs = spectra.reshape(spectra.shape[:-1] + (spectra.shape[-1] // 2, 2))
    partner = partner_of(grads)
    first = jnp.einsum('bmli,bmlq->liq', pairs[..., 0], grads)
    second = jnp.einsum('bmli,bmlq->liq', pairs[..., 1], partner)
    return first + second


def reference(saved_input, grad_output, legendre, quad_weight, mixing_weight):
    analysis = (legendre.astype(jnp.float32) * quad_weight[None, None, :]).astype(jnp.bfloat16)
    analysis_wide = analysis.astype(jnp.float32)
    spectra = jnp.einsum('mlj,bmjq->bmlq', analysis_wide, saved_input.astype(jnp.float32)).astype(jnp.bfloat16)
    grad_spectra = jnp.einsum('mlj,bmjq->bmlq', legendre.astype(jnp.float32), grad_output.astype(jnp.float32)).astype(jnp.bfloat16)
    batch = saved_input.shape[0]
    spec_wide = spectra.astype(jnp.float32)
    grad_wide = grad_spectra.astype(jnp.float32)
    spec_groups = spec_wide.reshape((N_DP, batch // N_DP) + spec_wide.shape[1:])
    grad_groups = grad_wide.reshape((N_DP, batch // N_DP) + grad_wide.shape[1:])

    def add_group(running, members):
        term = weight_terms(members[0], members[1]) / batch
        rounded = lax.optimization_barrier(term.astype(jnp.bfloat16))
        return running + rounded.astype(jnp.float32), None

    initial = jnp.zeros(mixing_weight.shape, jnp.float32)
    summed, unused = lax.scan(add_group, initial, (spec_groups, grad_groups))
    grad_weight = summed.astype(jnp.bfloat16)

    width = 2 * C // N_CHAN
    partner_wide = partner_of(grad_wide)
    grad_blocks = jnp.moveaxis(grad_wide.reshape(grad_wide.shape[:3] + (N_CHAN, width)), 3, 0)
    partner_blocks = jnp.moveaxis(partner_wide.reshape(partner_wide.shape[:3] + (N_CHAN, width)), 3, 0)
    weight_wide = mixing_weight.astype(jnp.float32)
    weight_blocks = jnp.moveaxis(weight_wide.reshape(weight_wide.shape[:2] + (N_CHAN, width)), 2, 0)

    def add_block(running, members):
        grads_block, partner_block, weights_block = members
        sum_real = jnp.einsum('bmlq,liq->bmli', grads_block, weights_block)
        sum_imag = jnp.einsum('bmlq,liq->bmli', partner_block, weights_block)
        term = jnp.stack([sum_real, sum_imag], axis=-1).reshape(running.shape)
        rounded = lax.optimization_barrier(term.astype(jnp.bfloat16))
        return running + rounded.astype(jnp.float32), None

    start_sum = jnp.zeros(spec_wide.shape, jnp.float32)
    spec_sum, unused_two = lax.scan(add_block, start_sum, (grad_blocks, partner_blocks, weight_blocks))
    grad_spec_in = spec_sum.astype(jnp.bfloat16)
    grad_input = jnp.einsum('mlj,bmlq->bmjq', analysis_wide, grad_spec_in.astype(jnp.float32)).astype(jnp.bfloat16)
    return (grad_weight, grad_input)
```

```python
import jax
import jax.numpy as jnp
from jax import lax
from jax.sharding import PartitionSpec as P

BF = jnp.bfloat16
F32 = jnp.float32


def lane_swap(width):
    row = lax.broadcasted_iota(jnp.int32, (width, width), 0)
    col = lax.broadcasted_iota(jnp.int32, (width, width), 1)
    up = (row == col + 1) & (col % 2 == 0)
    down = (col == row + 1) & (row % 2 == 0)
    return (up.astype(F32) - down.astype(F32)).astype(BF)


def to_planes(width):
    row = lax.broadcasted_iota(jnp.int32, (width, width), 0)
    col = lax.broadcasted_iota(jnp.int32, (width, width), 1)
    return ((row // 2 + (row % 2) * (width // 2)) == col).astype(BF)


def lanes(x, matrix):
    return jnp.einsum("...q,qp->...p", x, matrix, preferred_element_type=F32).astype(BF)


def shifted(x, axis, step):
    n = lax.axis_size(axis)
    return lax.ppermute(x, axis, [(i, (i + step) % n) for i in range(n)])


def pick(x, index):
    return lax.dynamic_index_in_dim(x, index, 0, keepdims=False)


def on_device(saved_input, grad_output, legendre, quad_weight, mixing_weight):
    local_lat = saved_input.shape[2]
    width = saved_input.shape[3]
    own_m, n_deg, n_lat = legendre.shape
    lat_size = lax.axis_size("lat")
    n_dp, n_chan = lax.axis_size("dp"), lax.axis_size("chan")
    my_dp, my_chan = lax.axis_index("dp"), lax.axis_index("chan")
    batch = saved_input.shape[0] * n_dp
    swap, planes = lane_swap(width), to_planes(width)

    share = 2 if own_m % 2 == 0 and n_dp % 2 == 0 else 1
    per = own_m // share
    half_of = my_dp % share
    orders = pick(legendre.reshape(share, per * n_deg, n_lat), half_of)
    by_lat = orders.T.reshape(lat_size, local_lat, per * n_deg)
    by_lat = lax.all_to_all(by_lat, "lat", split_axis=0, concat_axis=0, tiled=True)
    held = [by_lat]
    if share == 2:
        other = lax.ppermute(by_lat, "dp", [(i, i ^ 1) for i in range(n_dp)])
        first = half_of == 0
        held = [jnp.where(first, by_lat, other), jnp.where(first, other, by_lat)]
    held = [
        jnp.transpose(x.reshape(lat_size, local_lat, per, n_deg), (0, 2, 3, 1))
        for x in held
    ]
    table = jnp.concatenate(held, axis=1).reshape(lat_size * own_m, n_deg, local_lat)
    weights = lax.dynamic_slice_in_dim(
        quad_weight, lax.axis_index("lat") * local_lat, local_lat
    )
    analysis = (table.astype(F32) * weights[None, None, :]).astype(BF)

    def spectrum(tab, grid):
        part = jnp.einsum("mlj,bmjq->lbmq", tab, grid, preferred_element_type=F32)
        return lax.psum_scatter(part.astype(BF), "lat", scatter_dimension=0, tiled=True)

    grads = spectrum(table, grad_output)
    spectra = spectrum(analysis, saved_input)
    n_l, n_b, n_m = grads.shape[:3]
    rows = n_b * n_m

    flat = grads.reshape(n_l, rows, width)
    both = jnp.concatenate([flat, lanes(flat, swap)], axis=1)
    n_i = mixing_weight.shape[1]
    mine = n_i // n_chan
    split_weight = mixing_weight.reshape(n_l, n_chan, mine, width)
    terms = jnp.einsum("lrq,lciq->clri", both, split_weight, preferred_element_type=F32)
    terms = terms.astype(BF)
    total = pick(terms, my_chan).astype(F32)
    for step in range(1, n_chan):
        sent = pick(terms, (my_chan + step) % n_chan)
        total = total + shifted(sent, "chan", step).astype(F32)
    total = total.astype(BF)
    half = lanes_join(total.reshape(n_l, 2, rows, mine), planes)
    everyone = [flat] + [shifted(flat, "dp", step) for step in range(1, n_dp)]

    spectra, half, *everyone = lax.optimization_barrier((spectra, half, *everyone))
    spec_in = lax.all_gather(half, "lat", axis=0, tiled=True).reshape(-1, n_b, n_m, width)
    grad_input = jnp.einsum(
        "mlj,lbmq->bmjq", analysis, spec_in, preferred_element_type=F32
    ).astype(BF)

    block = n_i // n_dp
    size = min(block, mine)
    per_chan, per_block = mine // size, block // size
    planar = lanes(spectra.reshape(n_l, rows, width), planes)
    pieces = jnp.moveaxis(planar.reshape(n_l, rows, 2, per_chan, size), 3, 0)
    pieces = pieces.reshape(per_chan, n_l, rows, 2 * size)
    pieces = jnp.concatenate(
        [pieces] + [shifted(pieces, "chan", step) for step in range(1, n_chan)]
    )

    def piece(index):
        place = (my_chan - index // per_chan) % n_chan
        return pick(pieces, place * per_chan + index % per_chan)

    def block_of(owner):
        parts = [piece(owner * per_block + t) for t in range(per_block)]
        return jnp.stack(parts)

    ours = [block_of(my_dp)]
    for step in range(1, n_dp):
        ours.append(shifted(block_of((my_dp + step) % n_dp), "dp", step))
    left = jnp.stack(ours).reshape(n_dp, per_block, n_l, rows, 2, size)
    right = jnp.stack(everyone)
    right = jnp.stack([right, lanes(right, swap)])
    grad_weight = jnp.einsum(
        "dtlrpi,pdlrq->ltiq", left, right, preferred_element_type=F32
    ) / batch
    return (grad_weight.reshape(n_l, block, width).astype(BF), grad_input)


def lanes_join(parts, planes):
    n = parts.shape[-1]
    real = jnp.einsum("lri,qi->lrq", parts[:, 0], planes[:, :n], preferred_element_type=F32)
    imag = jnp.einsum("lri,qi->lrq", parts[:, 1], planes[:, n:], preferred_element_type=F32)
    return (real + imag).astype(BF)


def solution(mesh):
    in_specs = (
        P("dp", None, "lat", "chan"),
        P("dp", None, "lat", "chan"),
        P("lat", None, None),
        P(),
        P("lat", None, "chan"),
    )
    out_specs = (P("lat", "dp", "chan"), P("dp", None, "lat", "chan"))
    return jax.shard_map(
        on_device, mesh=mesh, in_specs=in_specs, out_specs=out_specs, check_vma=False
    )
```
